16 devices in a mesh: dp: 4 (over y, z, core), tp: 4 (over x).
Axes of the slice: x: 4, y: 2, z: 1, core: 2. Of those that a mesh axis runs over, the one named last changes fastest.
The devices are a block of a 4x4x8 slice.
Arguments:
- x: bfloat16 [512, 2048], P('dp'), parts along dimension 0
- w_gate: bfloat16 [2048, 5632], P(None, 'tp')
- w_up: bfloat16 [2048, 5632], P(None, 'tp')
- w_down: bfloat16 [5632, 2048], P('tp')
Outputs:
- output: bfloat16 [512, 2048], P('dp'), parts along dimension 0
There are 4 independent parts. The reference program is written for one: setup_inputs(seed, part) draws one part's arguments, and reference() takes and returns one part's arrays. A program takes and returns all parts, laid end to end along the dimension named above; an argument that names none is the same for every part.
All inputs are finite; a program needn't handle non-finite values.
Results may differ from the reference program's by a relative error of at most 0.016.
Values are sent between devices in bfloat16 or wider.
A program may use at most 768 MiB of HBM per device.

```python
import jax
import jax.numpy as jnp

ROWS = 128
D = 2048
FF = 5632


def setup_inputs(seed: int = 0, part: int = 0) -> dict:
    kx, kg, ku, kd = jax.random.split(jax.random.key(seed), 4)
    drawn = {
        "x": jax.random.normal(jax.random.fold_in(kx, part), (ROWS, D), jnp.float32),
        "w_gate": jax.random.normal(kg, (D, FF), jnp.float32) * D**-0.5,
        "w_up": jax.random.normal(ku, (D, FF), jnp.float32) * D**-0.5,
        "w_down": jax.random.normal(kd, (FF, D), jnp.float32) * FF**-0.5,
    }
    return {k: v.astype(jnp.bfloat16) for k, v in drawn.items()}


def reference(x, w_gate, w_up, w_down):
    gate = jnp.dot(x, w_gate, preferred_element_type=jnp.float32)
    up = jnp.dot(x, w_up, preferred_element_type=jnp.float32)
    hidden = (jax.nn.silu(gate) * up).astype(jnp.bfloat16)
    return jnp.dot(hidden, w_down, preferred_element_type=jnp.float32).astype(jnp.bfloat16)
```

```python
import functools

import jax
import jax.numpy as jnp
from jax import lax
from jax.experimental import pallas as pl
from jax.experimental.pallas import tpu as pltpu
from jax.sharding import PartitionSpec as P

MESH = pl.DeviceIdType.MESH
BLOCK = 256
SUBS = 2


def blocks(total, size):
    return [(at, min(size, total - at)) for at in range(0, total, size)]


def kernel(n, x_hbm, wg_hbm, wu_hbm, wd_hbm, y_ref, x_ref, wg, wu, wd, hidden, own, out_buf, in_buf,
           x_sem, gu_sem, wd_sem, send_sem, recv_sem, gather_send, gather_recv):
    me = lax.axis_index("tp")
    chunk = y_ref.shape[1] // n
    width = chunk // SUBS
    hops = [2, 1, 3, 0]

    def peer(hop):
        return lax.rem(me + hop, n)

    def columns(hop, sub):
        return pl.ds(pl.multiple_of(peer(hop) * chunk + sub * width, width), width)

    barrier = pltpu.get_barrier_semaphore()
    for hop in range(1, n):
        pl.semaphore_signal(barrier, inc=1, device_id={"tp": peer(hop)}, device_id_type=MESH)

    x_copy = pltpu.make_async_copy(x_hbm, x_ref, x_sem)
    x_copy.start()
    gu_copies = []
    for i, (at, size) in enumerate(blocks(hidden.shape[1], BLOCK)):
        cut = pl.ds(at, size)
        pair = [
            pltpu.make_async_copy(wg_hbm.at[:, cut], wg.at[:, cut], gu_sem.at[0, i]),
            pltpu.make_async_copy(wu_hbm.at[:, cut], wu.at[:, cut], gu_sem.at[1, i]),
        ]
        for copy in pair:
            copy.start()
        gu_copies.append(pair)
    wd_copies = {}
    for hop in hops:
        for sub in range(SUBS):
            copy = pltpu.make_async_copy(wd_hbm.at[:, columns(hop, sub)], wd.at[hop, sub], wd_sem.at[hop, sub])
            copy.start()
            wd_copies[hop, sub] = copy

    x_copy.wait()
    for (at, size), pair in zip(blocks(hidden.shape[1], BLOCK), gu_copies):
        cut = pl.ds(at, size)
        for copy in pair:
            copy.wait()
        gate = jnp.dot(x_ref[...], wg[:, cut], preferred_element_type=jnp.float32)
        up = jnp.dot(x_ref[...], wu[:, cut], preferred_element_type=jnp.float32)
        hidden[:, cut] = (jax.nn.silu(gate) * up).astype(jnp.bfloat16)

    pl.semaphore_wait(barrier, n - 1)

    terms = {}
    for hop in hops:
        for sub in range(SUBS):
            wd_copies[hop, sub].wait()
            term = jnp.dot(hidden[...], wd[hop, sub], preferred_element_type=jnp.float32)
            if hop == 0:
                own[sub] = term
                continue
            out_buf[hop - 1, sub] = term.astype(jnp.bfloat16)
            copy = pltpu.make_async_remote_copy(
                src_ref=out_buf.at[hop - 1, sub],
                dst_ref=in_buf.at[hop - 1, sub],
                send_sem=send_sem.at[hop - 1, sub],
                recv_sem=recv_sem.at[hop - 1, sub],
                device_id={"tp": peer(hop)},
                device_id_type=MESH,
            )
            copy.start()
            terms[hop, sub] = copy

    gathers = []
    for sub in range(SUBS):
        total = own[sub]
        for hop in hops[:-1]:
            terms[hop, sub].wait_recv()
            total += in_buf[hop - 1, sub].astype(jnp.float32)
        y_ref[:, columns(0, sub)] = total.astype(y_ref.dtype)
        for hop in hops[:-1]:
            copy = pltpu.make_async_remote_copy(
                src_ref=y_ref.at[:, columns(0, sub)],
                dst_ref=y_ref.at[:, columns(0, sub)],
                send_sem=gather_send.at[hop - 1, sub],
                recv_sem=gather_recv.at[hop - 1, sub],
                device_id={"tp": peer(hop)},
                device_id_type=MESH,
            )
            copy.start()
            gathers.append(copy)
    for copy in gathers:
        copy.wait_recv()
    for copy in list(terms.values()) + gathers:
        copy.wait_send()


def solution(mesh):
    n = mesh.shape["tp"]

    def step(x, w_gate, w_up, w_down):
        rows, depth = x.shape
        units, cols = w_down.shape
        width = cols // n // SUBS
        steps = len(blocks(units, BLOCK))
        dma = pltpu.SemaphoreType.DMA
        return pl.pallas_call(
            functools.partial(kernel, n),
            out_shape=pltpu.VMEM((rows, cols), jnp.bfloat16),
            in_specs=[pl.BlockSpec(memory_space=pl.ANY)] * 4,
            out_specs=pl.BlockSpec(memory_space=pltpu.VMEM),
            scratch_shapes=[
                pltpu.VMEM((rows, depth), jnp.bfloat16),
                pltpu.VMEM((depth, units), jnp.bfloat16),
                pltpu.VMEM((depth, units), jnp.bfloat16),
                pltpu.VMEM((n, SUBS, units, width), jnp.bfloat16),
                pltpu.VMEM((rows, units), jnp.bfloat16),
                pltpu.VMEM((SUBS, rows, width), jnp.float32),
                pltpu.VMEM((n - 1, SUBS, rows, width), jnp.bfloat16),
                pltpu.VMEM((n - 1, SUBS, rows, width), jnp.bfloat16),
                dma,
                dma((2, steps)),
                dma((n, SUBS)),
                dma((n - 1, SUBS)),
                dma((n - 1, SUBS)),
                dma((n - 1, SUBS)),
                dma((n - 1, SUBS)),
            ],
            compiler_params=pltpu.CompilerParams(collective_id=0, has_side_effects=True),
        )(x, w_gate, w_up, w_down)

    return jax.shard_map(
        step,
        mesh=mesh,
        in_specs=(P("dp", None), P(None, "tp"), P(None, "tp"), P("tp", None)),
        out_specs=P("dp", None),
        check_vma=False,
    )
```

```python
import functools

import jax
import jax.numpy as jnp
from jax import lax
from jax.experimental import pallas as pl
from jax.experimental.pallas import tpu as pltpu
from jax.sharding import PartitionSpec as P

MESH = pl.DeviceIdType.MESH
BLOCK = 256
SUBS = 2


def blocks(total, size):
    return [(at, min(size, total - at)) for at in range(0, total, size)]


def kernel(n, x_hbm, wg_hbm, wu_hbm, wd_hbm, y_ref, x_ref, wg, wu, wd, hidden, own, out_buf, in_buf,
           x_sem, gu_sem, wd_sem, send_sem, recv_sem, gather_send, gather_recv, order_sem):
    me = lax.axis_index("tp")
    chunk = y_ref.shape[1] // n
    width = chunk // SUBS
    hops = [2, 1, 3, 0]

    def peer(hop):
        return lax.rem(me + hop, n)

    def in_order():
        pl.semaphore_signal(order_sem, inc=1)

    def columns(hop, sub):
        return pl.ds(pl.multiple_of(peer(hop) * chunk + sub * width, width), width)

    x_copy = pltpu.make_async_copy(x_hbm, x_ref, x_sem)
    x_copy.start()
    in_order()
    gu_copies = []
    for i, (at, size) in enumerate(blocks(hidden.shape[1], BLOCK)):
        cut = pl.ds(at, size)
        pair = [
            pltpu.make_async_copy(wg_hbm.at[:, cut], wg.at[:, cut], gu_sem.at[0, i]),
            pltpu.make_async_copy(wu_hbm.at[:, cut], wu.at[:, cut], gu_sem.at[1, i]),
        ]
        for copy in pair:
            copy.start()
        in_order()
        gu_copies.append(pair)
    wd_copies = {}
    for hop in hops:
        for sub in range(SUBS):
            copy = pltpu.make_async_copy(wd_hbm.at[:, columns(hop, sub)], wd.at[hop, sub], wd_sem.at[hop, sub])
            copy.start()
            in_order()
            wd_copies[hop, sub] = copy
    pl.semaphore_wait(order_sem, 1 + len(gu_copies) + len(wd_copies))

    barrier = pltpu.get_barrier_semaphore()
    for hop in range(1, n):
        pl.semaphore_signal(barrier, inc=1, device_id={"tp": peer(hop)}, device_id_type=MESH)

    x_copy.wait()
    for (at, size), pair in zip(blocks(hidden.shape[1], BLOCK), gu_copies):
        cut = pl.ds(at, size)
        for copy in pair:
            copy.wait()
        gate = jnp.dot(x_ref[...], wg[:, cut], preferred_element_type=jnp.float32)
        up = jnp.dot(x_ref[...], wu[:, cut], preferred_element_type=jnp.float32)
        hidden[:, cut] = (jax.nn.silu(gate) * up).astype(jnp.bfloat16)

    pl.semaphore_wait(barrier, n - 1)

    terms = {}
    for hop in hops:
        for sub in range(SUBS):
            wd_copies[hop, sub].wait()
            term = jnp.dot(hidden[...], wd[hop, sub], preferred_element_type=jnp.float32)
            if hop == 0:
                own[sub] = term
                continue
            out_buf[hop - 1, sub] = term.astype(jnp.bfloat16)
            copy = pltpu.make_async_remote_copy(
                src_ref=out_buf.at[hop - 1, sub],
                dst_ref=in_buf.at[hop - 1, sub],
                send_sem=send_sem.at[hop - 1, sub],
                recv_sem=recv_sem.at[hop - 1, sub],
                device_id={"tp": peer(hop)},
                device_id_type=MESH,
            )
            copy.start()
            terms[hop, sub] = copy

    gathers = []
    for sub in range(SUBS):
        total = own[sub]
        for hop in hops[:-1]:
            terms[hop, sub].wait_recv()
            total += in_buf[hop - 1, sub].astype(jnp.float32)
        y_ref[:, columns(0, sub)] = total.astype(y_ref.dtype)
        for hop in hops[:-1]:
            copy = pltpu.make_async_remote_copy(
                src_ref=y_ref.at[:, columns(0, sub)],
                dst_ref=y_ref.at[:, columns(0, sub)],
                send_sem=gather_send.at[hop - 1, sub],
                recv_sem=gather_recv.at[hop - 1, sub],
                device_id={"tp": peer(hop)},
                device_id_type=MESH,
            )
            copy.start()
            gathers.append(copy)
    for copy in gathers:
        copy.wait_recv()
    for copy in list(terms.values()) + gathers:
        copy.wait_send()


def solution(mesh):
    n = mesh.shape["tp"]

    def step(x, w_gate, w_up, w_down):
        rows, depth = x.shape
        units, cols = w_down.shape
        width = cols // n // SUBS
        steps = len(blocks(units, BLOCK))
        dma = pltpu.SemaphoreType.DMA
        return pl.pallas_call(
            functools.partial(kernel, n),
            out_shape=pltpu.VMEM((rows, cols), jnp.bfloat16),
            in_specs=[pl.BlockSpec(memory_space=pl.ANY)] * 4,
            out_specs=pl.BlockSpec(memory_space=pltpu.VMEM),
            scratch_shapes=[
                pltpu.VMEM((rows, depth), jnp.bfloat16),
                pltpu.VMEM((depth, units), jnp.bfloat16),
                pltpu.VMEM((depth, units), jnp.bfloat16),
                pltpu.VMEM((n, SUBS, units, width), jnp.bfloat16),
                pltpu.VMEM((rows, units), jnp.bfloat16),
                pltpu.VMEM((SUBS, rows, width), jnp.float32),
                pltpu.VMEM((n - 1, SUBS, rows, width), jnp.bfloat16),
                pltpu.VMEM((n - 1, SUBS, rows, width), jnp.bfloat16),
                dma,
                dma((2, steps)),
                dma((n, SUBS)),
                dma((n - 1, SUBS)),
                dma((n - 1, SUBS)),
                dma((n - 1, SUBS)),
                dma((n - 1, SUBS)),
                pltpu.SemaphoreType.REGULAR,
            ],
            compiler_params=pltpu.CompilerParams(collective_id=0, has_side_effects=True),
        )(x, w_gate, w_up, w_down)

    return jax.shard_map(
        step,
        mesh=mesh,
        in_specs=(P("dp", None), P(None, "tp"), P(None, "tp"), P("tp", None)),
        out_specs=P("dp", None),
        check_vma=False,
    )
```

```python
import functools

import jax
import jax.numpy as jnp
from jax import lax
from jax.experimental import pallas as pl
from jax.experimental.pallas import tpu as pltpu
from jax.sharding import PartitionSpec as P

MESH = pl.DeviceIdType.MESH
BLOCK = 256
WIDTH = 128
HALVED = 3
WHOLE = 2


def both_sides(kind, pieces, *events):
    return [(*event, side, kind, i) for i in range(pieces) for event in [[e] for e in events] or [[]] for side in (0, 1)]


def merge(one, other):
    return [item for pair in zip(one, other) for item in pair] + one[len(other) :] + other[len(one) :]


STEPS = [(side, kind, 0, n) for kind, n in (("other", HALVED), ("kept", HALVED), ("whole", WHOLE)) for side in (0, 1)]
EVENTS = (
    both_sides("kept", HALVED, "join")
    + merge(both_sides("whole", WHOLE, "join"), both_sides("kept", HALVED, "finish"))
    + both_sides("whole", WHOLE, "finish")
)


def blocks(total, size):
    return [(at, min(size, total - at)) for at in range(0, total, size)]


def kernel(n, x_hbm, wg_hbm, wu_hbm, wd_hbm, y_ref, x_ref, wg, wu, wd, hidden, kept, out1, in1, out2, in2,
           x_sem, gu_sem, wd_sem, send1, recv1, send2, recv2, send3, recv3, order_sem):
    me = lax.axis_index("tp")
    span = y_ref.shape[1] // 2
    odd, far = lax.rem(me, 2), n - 1 - me
    near = me + 1 - 2 * odd
    first, second = (near, far), (far, near)
    half = (lax.rem((me + 1) // 2, 2), me // 2)

    def in_order():
        pl.semaphore_signal(order_sem, inc=1)

    def columns(side, kind, piece, pieces=1):
        if kind == "whole":
            return pl.ds(side * span + (2 * HALVED + piece) * WIDTH, pieces * WIDTH)
        at = half[side] if kind == "kept" else 1 - half[side]
        return pl.ds(pl.multiple_of(side * span + (at * HALVED + piece) * WIDTH, WIDTH), pieces * WIDTH)

    def send(src, dst, sends, recvs, to):
        copy = pltpu.make_async_remote_copy(
            src_ref=src, dst_ref=dst, send_sem=sends, recv_sem=recvs, device_id={"tp": to}, device_id_type=MESH
        )
        copy.start()
        return copy

    x_copy = pltpu.make_async_copy(x_hbm, x_ref, x_sem)
    x_copy.start()
    in_order()
    gu_copies = []
    for i, (at, size) in enumerate(blocks(hidden.shape[1], BLOCK)):
        cut = pl.ds(at, size)
        pair = [
            pltpu.make_async_copy(wg_hbm.at[:, cut], wg.at[:, cut], gu_sem.at[0, i]),
            pltpu.make_async_copy(wu_hbm.at[:, cut], wu.at[:, cut], gu_sem.at[1, i]),
        ]
        for copy in pair:
            copy.start()
        in_order()
        gu_copies.append(pair)
    wd_copies, at = [], 0
    for i, (side, kind, piece, pieces) in enumerate(STEPS):
        cut = pl.ds(at, pieces * WIDTH)
        copy = pltpu.make_async_copy(wd_hbm.at[:, columns(side, kind, piece, pieces)], wd.at[:, cut], wd_sem.at[i])
        copy.start()
        in_order()
        wd_copies.append((copy, cut))
        at += pieces * WIDTH
    pl.semaphore_wait(order_sem, 1 + len(gu_copies) + len(wd_copies))

    barrier = pltpu.get_barrier_semaphore()
    for neighbour in first:
        pl.semaphore_signal(barrier, inc=1, device_id={"tp": neighbour}, device_id_type=MESH)

    x_copy.wait()
    for (at, size), pair in zip(blocks(hidden.shape[1], BLOCK), gu_copies):
        cut = pl.ds(at, size)
        for copy in pair:
            copy.wait()
        gate = jnp.dot(x_ref[...], wg[:, cut], preferred_element_type=jnp.float32)
        up = jnp.dot(x_ref[...], wu[:, cut], preferred_element_type=jnp.float32)
        hidden[:, cut] = (jax.nn.silu(gate) * up).astype(jnp.bfloat16)

    pl.semaphore_wait(barrier, 2)

    swaps1, swaps2, swaps3 = {}, {}, {}

    def slot(side, kind, piece):
        return side, piece + (HALVED if kind == "whole" else 0)

    for (side, kind, piece, pieces), (wd_copy, cut) in zip(STEPS, wd_copies):
        wd_copy.wait()
        term = jnp.dot(hidden[...], wd[:, cut], preferred_element_type=jnp.float32)
        for i in range(pieces):
            at = slot(side, kind, piece + i)
            part = term[:, i * WIDTH : (i + 1) * WIDTH]
            if kind == "kept":
                kept[at] = part
            else:
                out1[at] = part.astype(jnp.bfloat16)
        if kind != "kept":
            for i in range(pieces):
                at = slot(side, kind, piece + i)
                swaps1[at] = send(out1.at[at], in1.at[at], send1.at[at], recv1.at[at], first[side])

    for event, side, kind, piece in EVENTS:
        at = slot(side, kind, piece)
        if event == "join":
            swaps1[at].wait_recv()
            mine = kept[at] if kind == "kept" else out1[at].astype(jnp.float32)
            out2[at] = (mine + in1[at].astype(jnp.float32)).astype(jnp.bfloat16)
            swaps2[at] = send(out2.at[at], in2.at[at], send2.at[at], recv2.at[at], second[side])
        else:
            swaps2[at].wait_recv()
            cut = columns(side, kind, piece)
            y_ref[:, cut] = (out2[at].astype(jnp.float32) + in2[at].astype(jnp.float32)).astype(y_ref.dtype)
            if kind == "kept":
                swaps3[at] = send(y_ref.at[:, cut], y_ref.at[:, cut], send3.at[at], recv3.at[at], first[side])
    for copy in swaps3.values():
        copy.wait_recv()
    for copy in [*swaps1.values(), *swaps2.values(), *swaps3.values()]:
        copy.wait_send()


def solution(mesh):
    n = mesh.shape["tp"]
    assert n == 4

    def step(x, w_gate, w_up, w_down):
        rows, depth = x.shape
        units, cols = w_down.shape
        steps = len(blocks(units, BLOCK))
        dma = pltpu.SemaphoreType.DMA
        count = HALVED + WHOLE
        assert cols == 2 * (2 * HALVED + WHOLE) * WIDTH
        pieces = pltpu.VMEM((2, count, rows, WIDTH), jnp.bfloat16)
        return pl.pallas_call(
            functools.partial(kernel, n),
            out_shape=pltpu.VMEM((rows, cols), jnp.bfloat16),
            in_specs=[pl.BlockSpec(memory_space=pl.ANY)] * 4,
            out_specs=pl.BlockSpec(memory_space=pltpu.VMEM),
            scratch_shapes=[
                pltpu.VMEM((rows, depth), jnp.bfloat16),
                pltpu.VMEM((depth, units), jnp.bfloat16),
                pltpu.VMEM((depth, units), jnp.bfloat16),
                pltpu.VMEM((units, cols), jnp.bfloat16),
                pltpu.VMEM((rows, units), jnp.bfloat16),
                pltpu.VMEM((2, HALVED, rows, WIDTH), jnp.float32),
                pieces,
                pieces,
                pieces,
                pieces,
                dma,
                dma((2, steps)),
                dma((len(STEPS),)),
                *[dma((2, count))] * 6,
                pltpu.SemaphoreType.REGULAR,
            ],
            compiler_params=pltpu.CompilerParams(collective_id=0, has_side_effects=True),
        )(x, w_gate, w_up, w_down)

    return jax.shard_map(
        step,
        mesh=mesh,
        in_specs=(P("dp", None), P(None, "tp"), P(None, "tp"), P("tp", None)),
        out_specs=P("dp", None),
        check_vma=False,
    )
```

```python
import functools

import jax
import jax.numpy as jnp
from jax import lax
from jax.experimental import pallas as pl
from jax.experimental.pallas import tpu as pltpu
from jax.sharding import PartitionSpec as P

MESH = pl.DeviceIdType.MESH
BLOCK = 256
HALVED = (128, 128, 128)
WHOLE = (256,)
SIDES = (1, 0)
GROUPS = (("other", 0, 3), ("kept", 0, 3), ("whole", 0, 1))


def both_sides(kind, event):
    pieces = WHOLE if kind == "whole" else HALVED
    return [(event, side, kind, i) for i in range(len(pieces)) for side in SIDES]


def merge(one, other):
    return [item for pair in zip(one, other) for item in pair] + one[len(other) :] + other[len(one) :]


STEPS = [(side, *group) for group in GROUPS for side in SIDES]
EVENTS = (
    both_sides("kept", "join")
    + merge(both_sides("whole", "join"), both_sides("kept", "finish"))
    + both_sides("whole", "finish")
)


def blocks(total, size):
    return [(at, min(size, total - at)) for at in range(0, total, size)]


def kernel(n, x_hbm, wg_hbm, wu_hbm, wd_hbm, y_ref, x_ref, wg, wu, wd, hidden, kept, out1, in1, out2, in2,
           x_sem, gu_sem, wd_sem, send1, recv1, send2, recv2, send3, recv3, order_sem):
    me = lax.axis_index("tp")
    span = y_ref.shape[1] // 2
    odd, far = lax.rem(me, 2), n - 1 - me
    near = me + 1 - 2 * odd
    first, second = (near, far), (far, near)
    half = (lax.rem((me + 1) // 2, 2), me // 2)

    def in_order():
        pl.semaphore_signal(order_sem, inc=1)

    def columns(side, kind, piece, pieces=1):
        if kind == "whole":
            return pl.ds(side * span + 2 * sum(HALVED) + sum(WHOLE[:piece]), sum(WHOLE[piece : piece + pieces]))
        at = half[side] if kind == "kept" else 1 - half[side]
        at = side * span + at * sum(HALVED) + sum(HALVED[:piece])
        return pl.ds(pl.multiple_of(at, 128), sum(HALVED[piece : piece + pieces]))

    def send(src, dst, sends, recvs, to):
        copy = pltpu.make_async_remote_copy(
            src_ref=src, dst_ref=dst, send_sem=sends, recv_sem=recvs, device_id={"tp": to}, device_id_type=MESH
        )
        copy.start()
        return copy

    x_copy = pltpu.make_async_copy(x_hbm, x_ref, x_sem)
    x_copy.start()
    in_order()
    gu_copies = []
    for i, (at, size) in enumerate(blocks(hidden.shape[1], BLOCK)):
        cut = pl.ds(at, size)
        pair = [
            pltpu.make_async_copy(wg_hbm.at[:, cut], wg.at[:, cut], gu_sem.at[0, i]),
            pltpu.make_async_copy(wu_hbm.at[:, cut], wu.at[:, cut], gu_sem.at[1, i]),
        ]
        for copy in pair:
            copy.start()
        in_order()
        gu_copies.append(pair)
    wd_copies, at = [], 0
    for i, (side, kind, piece, pieces) in enumerate(STEPS):
        where = columns(side, kind, piece, pieces)
        cut = pl.ds(at, where.size)
        copy = pltpu.make_async_copy(wd_hbm.at[:, where], wd.at[:, cut], wd_sem.at[i])
        copy.start()
        in_order()
        wd_copies.append((copy, cut))
        at += where.size
    pl.semaphore_wait(order_sem, 1 + len(gu_copies) + len(wd_copies))

    barrier = pltpu.get_barrier_semaphore()
    for neighbour in first:
        pl.semaphore_signal(barrier, inc=1, device_id={"tp": neighbour}, device_id_type=MESH)

    x_copy.wait()
    for (at, size), pair in zip(blocks(hidden.shape[1], BLOCK), gu_copies):
        cut = pl.ds(at, size)
        for copy in pair:
            copy.wait()
        gate = jnp.dot(x_ref[...], wg[:, cut], preferred_element_type=jnp.float32)
        up = jnp.dot(x_ref[...], wu[:, cut], preferred_element_type=jnp.float32)
        hidden[:, cut] = (jax.nn.silu(gate) * up).astype(jnp.bfloat16)

    pl.semaphore_wait(barrier, 2)

    swaps1, swaps2, swaps3 = {}, {}, {}

    def slot(side, kind, piece):
        return side, piece + (len(HALVED) if kind == "whole" else 0)

    for (side, kind, first_piece, pieces), (wd_copy, cut) in zip(STEPS, wd_copies):
        wd_copy.wait()
        term = jnp.dot(hidden[...], wd[:, cut], preferred_element_type=jnp.float32)
        at = 0
        for i in range(first_piece, first_piece + pieces):
            a, b = slot(side, kind, i)
            width = (WHOLE if kind == "whole" else HALVED)[i]
            part = term[:, at : at + width]
            at += width
            if kind == "kept":
                kept[a][b][...] = part
            else:
                out1[a][b][...] = part.astype(jnp.bfloat16)
        if kind != "kept":
            for i in range(first_piece, first_piece + pieces):
                a, b = at = slot(side, kind, i)
                swaps1[at] = send(out1[a][b], in1[a][b], send1.at[at], recv1.at[at], first[side])

    for event, side, kind, piece in EVENTS:
        a, b = at = slot(side, kind, piece)
        if event == "join":
            swaps1[at].wait_recv()
            mine = kept[a][b][...] if kind == "kept" else out1[a][b][...].astype(jnp.float32)
            out2[a][b][...] = (mine + in1[a][b][...].astype(jnp.float32)).astype(jnp.bfloat16)
            swaps2[at] = send(out2[a][b], in2[a][b], send2.at[at], recv2.at[at], second[side])
        else:
            swaps2[at].wait_recv()
            cut = columns(side, kind, piece)
            y_ref[:, cut] = (out2[a][b][...].astype(jnp.float32) + in2[a][b][...].astype(jnp.float32)).astype(y_ref.dtype)
            if kind == "kept":
                swaps3[at] = send(y_ref.at[:, cut], y_ref.at[:, cut], send3.at[at], recv3.at[at], first[side])
    for copy in swaps3.values():
        copy.wait_recv()
    for copy in [*swaps1.values(), *swaps2.values(), *swaps3.values()]:
        copy.wait_send()


def solution(mesh):
    n = mesh.shape["tp"]
    assert n == 4

    def step(x, w_gate, w_up, w_down):
        rows, depth = x.shape
        units, cols = w_down.shape
        steps = len(blocks(units, BLOCK))
        dma = pltpu.SemaphoreType.DMA
        widths = HALVED + WHOLE
        assert cols == 2 * (2 * sum(HALVED) + sum(WHOLE))
        pieces = [[pltpu.VMEM((rows, width), jnp.bfloat16) for width in widths] for side in (0, 1)]
        return pl.pallas_call(
            functools.partial(kernel, n),
            out_shape=pltpu.VMEM((rows, cols), jnp.bfloat16),
            in_specs=[pl.BlockSpec(memory_space=pl.ANY)] * 4,
            out_specs=pl.BlockSpec(memory_space=pltpu.VMEM),
            scratch_shapes=[
                pltpu.VMEM((rows, depth), jnp.bfloat16),
                pltpu.VMEM((depth, units), jnp.bfloat16),
                pltpu.VMEM((depth, units), jnp.bfloat16),
                pltpu.VMEM((units, cols), jnp.bfloat16),
                pltpu.VMEM((rows, units), jnp.bfloat16),
                [[pltpu.VMEM((rows, width), jnp.float32) for width in HALVED] for side in (0, 1)],
                pieces,
                pieces,
                pieces,
                pieces,
                dma,
                dma((2, steps)),
                dma((len(STEPS),)),
                *[dma((2, len(widths)))] * 6,
                pltpu.SemaphoreType.REGULAR,
            ],
            compiler_params=pltpu.CompilerParams(collective_id=0, has_side_effects=True),
        )(x, w_gate, w_up, w_down)

    return jax.shard_map(
        step,
        mesh=mesh,
        in_specs=(P("dp", None), P(None, "tp"), P(None, "tp"), P("tp", None)),
        out_specs=P("dp", None),
        check_vma=False,
    )
```

```python
import functools

import jax
import jax.numpy as jnp
from jax import lax
from jax.experimental import pallas as pl
from jax.experimental.pallas import tpu as pltpu
from jax.sharding import PartitionSpec as P

MESH = pl.DeviceIdType.MESH
BLOCKS = (384, 512, 256, 256)
HALVED = ((128, 128, 128), (128, 128, 128))
WHOLE = ((128,), (384,))
SIDES = (1, 0)
SPANS = [(sum(BLOCKS[:i]), size) for i, size in enumerate(BLOCKS)]


def of_kind(kind, *event):
    pieces = [(*event, side, kind, i) for side in SIDES for i in range(len((WHOLE if kind == "whole" else HALVED)[side]))]
    return sorted(pieces, key=lambda piece: piece[-1])


def merge(one, other):
    return [item for pair in zip(one, other) for item in pair] + one[len(other) :] + other[len(one) :]


STEPS = [
    (side, kind, 0, len((WHOLE if kind == "whole" else HALVED)[side])) for kind in ("other", "kept", "whole") for side in SIDES
]
EVENTS = (
    of_kind("kept", "join")
    + merge(of_kind("whole", "join"), of_kind("kept", "finish"))
    + of_kind("whole", "finish")
)


def kernel(n, x_hbm, wg_hbm, wu_hbm, wd_hbm, y_ref, x_ref, wg, wu, wd, hidden, kept, out1, in1, out2, in2,
           x_sem, gu_sem, wd_sem, send1, recv1, send2, recv2, send3, recv3, order_sem):
    me = lax.axis_index("tp")
    odd, far = lax.rem(me, 2), n - 1 - me
    near = me + 1 - 2 * odd
    first, second = (near, far), (far, near)
    half = (lax.rem((me + 1) // 2, 2), me // 2)

    def in_order():
        pl.semaphore_signal(order_sem, inc=1)

    def columns(side, kind, piece, pieces=1):
        start = side * (2 * sum(HALVED[0]) + sum(WHOLE[0]))
        if kind == "whole":
            widths = WHOLE[side]
            return pl.ds(start + 2 * sum(HALVED[side]) + sum(widths[:piece]), sum(widths[piece : piece + pieces]))
        widths = HALVED[side]
        at = half[side] if kind == "kept" else 1 - half[side]
        at = start + at * sum(widths) + sum(widths[:piece])
        return pl.ds(pl.multiple_of(at, 128), sum(widths[piece : piece + pieces]))

    def send(src, dst, sends, recvs, to):
        copy = pltpu.make_async_remote_copy(
            src_ref=src, dst_ref=dst, send_sem=sends, recv_sem=recvs, device_id={"tp": to}, device_id_type=MESH
        )
        copy.start()
        return copy

    x_copy = pltpu.make_async_copy(x_hbm, x_ref, x_sem)
    x_copy.start()
    in_order()
    gu_copies = []
    for i, (at, size) in enumerate(SPANS):
        cut = pl.ds(at, size)
        pair = [
            pltpu.make_async_copy(wg_hbm.at[:, cut], wg.at[:, cut], gu_sem.at[0, i]),
            pltpu.make_async_copy(wu_hbm.at[:, cut], wu.at[:, cut], gu_sem.at[1, i]),
        ]
        for copy in pair:
            copy.start()
        in_order()
        gu_copies.append(pair)
    wd_copies, at = [], 0
    for i, (side, kind, piece, pieces) in enumerate(STEPS):
        where = columns(side, kind, piece, pieces)
        cut = pl.ds(at, where.size)
        copy = pltpu.make_async_copy(wd_hbm.at[:, where], wd.at[:, cut], wd_sem.at[i])
        copy.start()
        in_order()
        wd_copies.append((copy, cut))
        at += where.size
    pl.semaphore_wait(order_sem, 1 + len(gu_copies) + len(wd_copies))

    barrier = pltpu.get_barrier_semaphore()
    for neighbour in first:
        pl.semaphore_signal(barrier, inc=1, device_id={"tp": neighbour}, device_id_type=MESH)

    x_copy.wait()
    for (at, size), pair in zip(SPANS, gu_copies):
        cut = pl.ds(at, size)
        for copy in pair:
            copy.wait()
        gate = jnp.dot(x_ref[...], wg[:, cut], preferred_element_type=jnp.float32)
        up = jnp.dot(x_ref[...], wu[:, cut], preferred_element_type=jnp.float32)
        hidden[:, cut] = (jax.nn.silu(gate) * up).astype(jnp.bfloat16)

    pl.semaphore_wait(barrier, 2)

    swaps1, swaps2, swaps3 = {}, {}, {}

    def slot(side, kind, piece):
        return side, piece + (len(HALVED[side]) if kind == "whole" else 0)

    for (side, kind, first_piece, pieces), (wd_copy, cut) in zip(STEPS, wd_copies):
        wd_copy.wait()
        term = jnp.dot(hidden[...], wd[:, cut], preferred_element_type=jnp.float32)
        at = 0
        for i in range(first_piece, first_piece + pieces):
            a, b = slot(side, kind, i)
            width = (WHOLE if kind == "whole" else HALVED)[side][i]
            part = term[:, at : at + width]
            at += width
            if kind == "kept":
                kept[a][b][...] = part
            else:
                out1[a][b][...] = part.astype(jnp.bfloat16)
        if kind != "kept":
            for i in range(first_piece, first_piece + pieces):
                a, b = at = slot(side, kind, i)
                swaps1[at] = send(out1[a][b], in1[a][b], send1.at[at], recv1.at[at], first[side])

    for event, side, kind, piece in EVENTS:
        a, b = at = slot(side, kind, piece)
        if event == "join":
            swaps1[at].wait_recv()
            mine = kept[a][b][...] if kind == "kept" else out1[a][b][...].astype(jnp.float32)
            out2[a][b][...] = (mine + in1[a][b][...].astype(jnp.float32)).astype(jnp.bfloat16)
            swaps2[at] = send(out2[a][b], in2[a][b], send2.at[at], recv2.at[at], second[side])
        else:
            swaps2[at].wait_recv()
            cut = columns(side, kind, piece)
            y_ref[:, cut] = (out2[a][b][...].astype(jnp.float32) + in2[a][b][...].astype(jnp.float32)).astype(y_ref.dtype)
            if kind == "kept":
                swaps3[at] = send(y_ref.at[:, cut], y_ref.at[:, cut], send3.at[at], recv3.at[at], first[side])
    for copy in swaps3.values():
        copy.wait_recv()
    for copy in [*swaps1.values(), *swaps2.values(), *swaps3.values()]:
        copy.wait_send()


def solution(mesh):
    n = mesh.shape["tp"]
    assert n == 4

    def step(x, w_gate, w_up, w_down):
        rows, depth = x.shape
        units, cols = w_down.shape
        assert units == sum(BLOCKS)
        dma = pltpu.SemaphoreType.DMA
        widths = [HALVED[side] + WHOLE[side] for side in (0, 1)]
        assert cols == sum(sum(HALVED[side]) + sum(widths[side]) for side in (0, 1))
        pieces = [[pltpu.VMEM((rows, width), jnp.bfloat16) for width in widths[side]] for side in (0, 1)]
        return pl.pallas_call(
            functools.partial(kernel, n),
            out_shape=pltpu.VMEM((rows, cols), jnp.bfloat16),
            in_specs=[pl.BlockSpec(memory_space=pl.ANY)] * 4,
            out_specs=pl.BlockSpec(memory_space=pltpu.VMEM),
            scratch_shapes=[
                pltpu.VMEM((rows, depth), jnp.bfloat16),
                pltpu.VMEM((depth, units), jnp.bfloat16),
                pltpu.VMEM((depth, units), jnp.bfloat16),
                pltpu.VMEM((units, cols), jnp.bfloat16),
                pltpu.VMEM((rows, units), jnp.bfloat16),
                [[pltpu.VMEM((rows, width), jnp.float32) for width in HALVED[side]] for side in (0, 1)],
                pieces,
                pieces,
                pieces,
                pieces,
                dma,
                dma((2, len(BLOCKS))),
                dma((len(STEPS),)),
                *[dma((2, max(map(len, widths))))] * 6,
                pltpu.SemaphoreType.REGULAR,
            ],
            compiler_params=pltpu.CompilerParams(collective_id=0, has_side_effects=True),
        )(x, w_gate, w_up, w_down)

    return jax.shard_map(
        step,
        mesh=mesh,
        in_specs=(P("dp", None), P(None, "tp"), P(None, "tp"), P("tp", None)),
        out_specs=P("dp", None),
        check_vma=False,
    )
```

```python
import functools

import jax
import jax.numpy as jnp
from jax import lax
from jax.experimental import pallas as pl
from jax.experimental.pallas import tpu as pltpu
from jax.sharding import PartitionSpec as P

MESH = pl.DeviceIdType.MESH
BLOCKS = (384, 512, 256, 256)
HALVED = ((128, 128, 128), (128, 128, 128))
WHOLE = ((128,), (384,))
SIDES = (1, 0)
SPANS = [(sum(BLOCKS[:i]), size) for i, size in enumerate(BLOCKS)]


def of_kind(kind, *event):
    pieces = [(*event, side, kind, i) for side in SIDES for i in range(len((WHOLE if kind == "whole" else HALVED)[side]))]
    return sorted(pieces, key=lambda piece: piece[-1])


def merge(one, other):
    return [item for pair in zip(one, other) for item in pair] + one[len(other) :] + other[len(one) :]


STEPS = [(1, "other", 0, 1), (1, "other", 1, 2), (0, "other", 0, 3)] + [
    (side, kind, 0, len((WHOLE if kind == "whole" else HALVED)[side])) for kind in ("kept", "whole") for side in SIDES
]
EVENTS = (
    of_kind("kept", "join")
    + merge(of_kind("whole", "join"), of_kind("kept", "finish"))
    + of_kind("whole", "finish")
)


def kernel(n, x_hbm, wg_hbm, wu_hbm, wd_hbm, y_ref, x_ref, wg, wu, wd, hidden, kept, out1, in1, out2, in2,
           x_sem, gu_sem, wd_sem, send1, recv1, send2, recv2, send3, recv3, order_sem):
    me = lax.axis_index("tp")
    odd, far = lax.rem(me, 2), n - 1 - me
    near = me + 1 - 2 * odd
    first, second = (near, far), (far, near)
    half = (lax.rem((me + 1) // 2, 2), me // 2)

    def in_order():
        pl.semaphore_signal(order_sem, inc=1)

    def columns(side, kind, piece, pieces=1):
        start = side * (2 * sum(HALVED[0]) + sum(WHOLE[0]))
        if kind == "whole":
            widths = WHOLE[side]
            return pl.ds(start + 2 * sum(HALVED[side]) + sum(widths[:piece]), sum(widths[piece : piece + pieces]))
        widths = HALVED[side]
        at = half[side] if kind == "kept" else 1 - half[side]
        at = start + at * sum(widths) + sum(widths[:piece])
        return pl.ds(pl.multiple_of(at, 128), sum(widths[piece : piece + pieces]))

    def send(src, dst, sends, recvs, to):
        copy = pltpu.make_async_remote_copy(
            src_ref=src, dst_ref=dst, send_sem=sends, recv_sem=recvs, device_id={"tp": to}, device_id_type=MESH
        )
        copy.start()
        return copy

    x_copy = pltpu.make_async_copy(x_hbm, x_ref, x_sem)
    gu_copies = []
    for i, (at, size) in enumerate(SPANS):
        cut = pl.ds(at, size)
        pair = [
            pltpu.make_async_copy(wg_hbm.at[:, cut], wg.at[:, cut], gu_sem.at[0, i]),
            pltpu.make_async_copy(wu_hbm.at[:, cut], wu.at[:, cut], gu_sem.at[1, i]),
        ]
        for copy in pair:
            copy.start()
        if i == 0:
            x_copy.start()
        in_order()
        gu_copies.append(pair)
    wd_copies, at = [], 0
    for i, (side, kind, piece, pieces) in enumerate(STEPS):
        where = columns(side, kind, piece, pieces)
        cut = pl.ds(at, where.size)
        copy = pltpu.make_async_copy(wd_hbm.at[:, where], wd.at[:, cut], wd_sem.at[i])
        copy.start()
        in_order()
        wd_copies.append((copy, cut))
        at += where.size
    pl.semaphore_wait(order_sem, len(gu_copies) + len(wd_copies))

    barrier = pltpu.get_barrier_semaphore()
    for neighbour in first:
        pl.semaphore_signal(barrier, inc=1, device_id={"tp": neighbour}, device_id_type=MESH)

    x_copy.wait()
    for (at, size), pair in zip(SPANS, gu_copies):
        cut = pl.ds(at, size)
        for copy in pair:
            copy.wait()
        gate = jnp.dot(x_ref[...], wg[:, cut], preferred_element_type=jnp.float32)
        up = jnp.dot(x_ref[...], wu[:, cut], preferred_element_type=jnp.float32)
        hidden[:, cut] = (jax.nn.silu(gate) * up).astype(jnp.bfloat16)

    pl.semaphore_wait(barrier, 2)

    swaps1, swaps2, swaps3 = {}, {}, {}

    def slot(side, kind, piece):
        return side, piece + (len(HALVED[side]) if kind == "whole" else 0)

    for (side, kind, first_piece, pieces), (wd_copy, cut) in zip(STEPS, wd_copies):
        wd_copy.wait()
        term = jnp.dot(hidden[...], wd[:, cut], preferred_element_type=jnp.float32)
        at = 0
        for i in range(first_piece, first_piece + pieces):
            a, b = slot(side, kind, i)
            width = (WHOLE if kind == "whole" else HALVED)[side][i]
            part = term[:, at : at + width]
            at += width
            if kind == "kept":
                kept[a][b][...] = part
            else:
                out1[a][b][...] = part.astype(jnp.bfloat16)
        if kind != "kept":
            for i in range(first_piece, first_piece + pieces):
                a, b = at = slot(side, kind, i)
                swaps1[at] = send(out1[a][b], in1[a][b], send1.at[at], recv1.at[at], first[side])

    for event, side, kind, piece in EVENTS:
        a, b = at = slot(side, kind, piece)
        if event == "join":
            swaps1[at].wait_recv()
            mine = kept[a][b][...] if kind == "kept" else out1[a][b][...].astype(jnp.float32)
            out2[a][b][...] = (mine + in1[a][b][...].astype(jnp.float32)).astype(jnp.bfloat16)
            swaps2[at] = send(out2[a][b], in2[a][b], send2.at[at], recv2.at[at], second[side])
        else:
            swaps2[at].wait_recv()
            cut = columns(side, kind, piece)
            y_ref[:, cut] = (out2[a][b][...].astype(jnp.float32) + in2[a][b][...].astype(jnp.float32)).astype(y_ref.dtype)
            if kind == "kept":
                swaps3[at] = send(y_ref.at[:, cut], y_ref.at[:, cut], send3.at[at], recv3.at[at], first[side])
    for copy in swaps3.values():
        copy.wait_recv()
    for copy in [*swaps1.values(), *swaps2.values(), *swaps3.values()]:
        copy.wait_send()


def solution(mesh):
    n = mesh.shape["tp"]
    assert n == 4

    def step(x, w_gate, w_up, w_down):
        rows, depth = x.shape
        units, cols = w_down.shape
        assert units == sum(BLOCKS)
        dma = pltpu.SemaphoreType.DMA
        widths = [HALVED[side] + WHOLE[side] for side in (0, 1)]
        assert cols == sum(sum(HALVED[side]) + sum(widths[side]) for side in (0, 1))
        pieces = [[pltpu.VMEM((rows, width), jnp.bfloat16) for width in widths[side]] for side in (0, 1)]
        return pl.pallas_call(
            functools.partial(kernel, n),
            out_shape=pltpu.VMEM((rows, cols), jnp.bfloat16),
            in_specs=[pl.BlockSpec(memory_space=pl.ANY)] * 4,
            out_specs=pl.BlockSpec(memory_space=pltpu.VMEM),
            scratch_shapes=[
                pltpu.VMEM((rows, depth), jnp.bfloat16),
                pltpu.VMEM((depth, units), jnp.bfloat16),
                pltpu.VMEM((depth, units), jnp.bfloat16),
                pltpu.VMEM((units, cols), jnp.bfloat16),
                pltpu.VMEM((rows, units), jnp.bfloat16),
                [[pltpu.VMEM((rows, width), jnp.float32) for width in HALVED[side]] for side in (0, 1)],
                pieces,
                pieces,
                pieces,
                pieces,
                dma,
                dma((2, len(BLOCKS))),
                dma((len(STEPS),)),
                *[dma((2, max(map(len, widths))))] * 6,
                pltpu.SemaphoreType.REGULAR,
            ],
            compiler_params=pltpu.CompilerParams(collective_id=0, has_side_effects=True),
        )(x, w_gate, w_up, w_down)

    return jax.shard_map(
        step,
        mesh=mesh,
        in_specs=(P("dp", None), P(None, "tp"), P(None, "tp"), P("tp", None)),
        out_specs=P("dp", None),
        check_vma=False,
    )
```
